32 devices in a mesh: group: 2 (over y), view: 4 (over z), depth: 2 (over x), row: 2 (over core).
Axes of the slice: x: 2, y: 2, z: 4, core: 2. Of those that a mesh axis runs over, the one named last changes fastest.
Arguments:
- features: float32 [4, 32, 8, 512], P('view', None, ('group', 'row')), parts along dimension 2, may hold values from -6 to 6
- cotangent: float32 [8, 32, 8, 512], P('depth', 'view', ('group', 'row')), parts along dimension 2, may hold values from -6 to 6
- src_row: int32 [4, 8, 8, 512], P('view', 'depth', ('group', 'row')), parts along dimension 2, may hold values from -2 to 4, as said below
- src_col: int32 [4, 8, 8, 512], P('view', 'depth', ('group', 'row')), parts along dimension 2, may hold values from 0 to 510
- fractions: int32 [2, 4, 8, 8, 512], P(None, 'view', 'depth', ('group', 'row')), parts along dimension 3, may hold values from 0 to 256
Outputs:
- grad_features: float32 [4, 32, 8, 512], P('view', None, ('group', 'row'), 'depth'), parts along dimension 2
The draws below stay inside these ranges and needn't reach their ends.
There are 2 independent parts, one for each index of `group`. The reference program is written for one: setup_inputs(seed, part) draws one part's arguments, and reference() takes and returns one part's arrays. A program takes and returns all parts, laid end to end along the dimension named above; each array names one. Nothing has to cross between parts.
Inputs may be any that keep to these rules, and one draw needn't show every extreme that they name: src_row[v, d, y, x] lies between y - 2 and y + 1.
All inputs are finite; a program needn't handle non-finite values.
Results may differ from the reference program's by a relative error of at most 0.0003.
Values sent between devices are 32-bit elements; how exact they have to be, the bound alone decides.
A program may use at most 64 MiB of HBM per device.

```python
import jax
import jax.numpy as jnp
from jax import lax

C = 32
WC = 512
HALO = 2
VIEWS = 4
DEPTHS = 8
H = 4


def draw_src_row(key, part):
    shape_all = (VIEWS, DEPTHS, H, WC)
    offsets = jax.random.randint(jax.random.fold_in(key, 7), shape_all, -HALO, HALO)
    offsets = offsets.at[:, :, :, 0].set(-HALO).at[:, :, :, 1].set(HALO - 1)
    pixel_rows = lax.broadcasted_iota(jnp.int32, shape_all, 2)
    return (pixel_rows + offsets).astype(jnp.int32)


def draw_src_col(key, part):
    shape_all = (VIEWS, DEPTHS, H, WC)
    key_one, key_two = jax.random.split(jax.random.fold_in(key, 11))
    shifts = jax.random.randint(key_one, (VIEWS, 1, 1, 1), 0, 5)
    jitter = jax.random.randint(key_two, shape_all, -2, 3)
    planes = lax.broadcasted_iota(jnp.int32, shape_all, 1)
    columns = lax.broadcasted_iota(jnp.int32, shape_all, 3)
    values = jnp.clip(columns - (planes + 1) * shifts + jitter, 0, WC - 2)
    values = values.at[:, :, 0, 0].set(0).at[:, :, 0, WC - 1].set(WC - 2)
    return values.astype(jnp.int32)


def with_ends(entries, rng, least, high):
    longest = entries.shape.index(max(entries.shape))
    spots = []
    for shift in (0, 1):
        where = [jax.random.randint(jax.random.fold_in(rng, axis), (), 0, length) for axis, length in enumerate(entries.shape)]
        where[longest] = (where[longest] + shift) % entries.shape[longest]
        spots.append(tuple(where))
    return entries.at[spots[0]].set(least).at[spots[1]].set(high)


def block_levels(own_key, extent, shards, low, top_value):
    factor_of, own = 1.0, jax.random.fold_in(own_key, 6)
    for axis_at, shards_of in shards:
        heights = jnp.exp(jax.random.uniform(jax.random.fold_in(own, axis_at), (shards_of,), jnp.float32, low / len(shards), top_value / len(shards)))
        factor_of = factor_of * jnp.repeat(heights, extent[axis_at] // shards_of).reshape([-1 if axis == axis_at else 1 for axis in range(len(extent))])
    return factor_of


def scatter_about(key, shape, scale, limit, pieces=(), kind=jnp.bfloat16):
    entries = scale * jax.random.normal(key, shape, jnp.float32)
    if pieces:
        entries = entries * block_levels(key, shape, pieces, -0.22, 0.18)
    return jnp.clip(entries, -limit, limit).astype(kind)


def setup_inputs(seed: int = 0, part: int = 0) -> dict:
    key_list = jax.random.split(jax.random.key(seed), 6)
    part_keys = jax.random.split(jax.random.fold_in(key_list[5], part), 6)
    return {
        "features": scatter_about(part_keys[0], (VIEWS, C, H, WC), 1.0, 6.0, ((0, 4), (2, 2)), jnp.float32),
        "cotangent": scatter_about(part_keys[1], (DEPTHS, C, H, WC), (VIEWS / 8), 6.0, ((0, 2), (1, 4), (2, 2)), jnp.float32),
        "src_row": draw_src_row(jax.random.fold_in(jax.random.fold_in(key_list[5], part), 71), part),
        "src_col": draw_src_col(jax.random.fold_in(jax.random.fold_in(key_list[5], part), 71), part),
        "fractions": with_ends(jax.random.randint(part_keys[4], (2, VIEWS, DEPTHS, H, WC), 0, 257), jax.random.fold_in(part_keys[4], 1), 0, 256).astype(jnp.int32),
    }


def sample(flattened, flat_index, frac_row, frac_col, width):
    def corner(shift_by):
        return jnp.take(flattened, flat_index + shift_by, axis=1)
    upper_mix = (1.0 - frac_col) * corner(0) + frac_col * corner(1)
    lower_mix = (1.0 - frac_col) * corner(width) + frac_col * corner(width + 1)
    mixed = (1.0 - frac_row) * upper_mix + frac_row * lower_mix
    return jnp.transpose(mixed, (1, 0, 2, 3))


def spread(grad_warp, flat_index, frac_row, frac_col, width, length):
    moved = jnp.transpose(grad_warp, (1, 0, 2, 3))
    channels = moved.shape[0]
    upper_part = (1.0 - frac_row) * moved
    lower_part = frac_row * moved
    result = jnp.zeros((channels, length), jnp.float32)
    result = result.at[:, flat_index].add((1.0 - frac_col) * upper_part)
    result = result.at[:, flat_index + 1].add(frac_col * upper_part)
    result = result.at[:, flat_index + width].add((1.0 - frac_col) * lower_part)
    result = result.at[:, flat_index + width + 1].add(frac_col * lower_part)
    return result


def reference(features, cotangent, src_row, src_col, fractions):
    padded = jnp.pad(features, ((0, 0), (0, 0), (HALO, HALO), (0, 0)))
    length = (H + 2 * HALO) * WC
    flattened_all = padded.reshape(VIEWS, C, length)
    weights = fractions.astype(jnp.float32) / 256.0

    def warp_view(index_view):
        flat_index = ((src_row[index_view] + HALO) * WC + src_col[index_view]).astype(jnp.int32)
        warped = sample(flattened_all[index_view], flat_index, weights[0, index_view], weights[1, index_view], WC)
        return warped, flat_index

    def accumulate(index_view, running):
        return running + warp_view(index_view)[0]

    view_sum = lax.fori_loop(0, VIEWS, accumulate, jnp.zeros((DEPTHS, C, H, WC), jnp.float32))
    average = view_sum / VIEWS
    factor = 2.0 / VIEWS

    def backward_view(index_view):
        warped, flat_index = warp_view(index_view)
        grad_warp = factor * cotangent * (warped - average)
        spread_out = spread(grad_warp, flat_index, weights[0, index_view], weights[1, index_view], WC, length)
        return spread_out.reshape(C, H + 2 * HALO, WC)[:, HALO:HALO + H]

    return lax.map(backward_view, jnp.arange(VIEWS, dtype=jnp.int32))
```

```python
import functools

import jax
import jax.numpy as jnp
from jax import lax
from jax.experimental import pallas as pl
from jax.experimental.pallas import tpu as pltpu
from jax.sharding import PartitionSpec as P

MESH = pl.DeviceIdType.MESH
F32 = jnp.float32
BF16 = jnp.bfloat16
SPAN = 128
STRIDE = SPAN - 1
COLS = 256
UNROLL = 4


def split(value, axis):
    high = value.astype(BF16)
    low = (value - high.astype(F32)).astype(BF16)
    return jnp.concatenate([high, low], axis=axis)


def kernel(
    sizes, feat, cot, srow, scol, frac, out,
    fbuf, sbuf, qbuf, wbuf, cbuf, cotv, cotg, flat, mats, moved, warp, wsum, outbuf, pbuf, red, inbuf,
    local_sem, f_send, f_recv, p_send, p_recv, i_send, i_recv, d_send, d_recv, o_send, o_recv,
):
    views, depths, rows, cc, planes, rl, width = sizes
    me = lax.axis_index("view")
    mx = lax.axis_index("depth")
    mr = lax.axis_index("row")
    height = rows * rl
    wx = width // depths
    lines = planes * rl
    spans = (width - 1) // STRIDE + 1
    factor = 2.0 / views
    siblings = [(dx, dr) for dx in range(depths) for dr in range(rows) if dx or dr]

    def view_at(step):
        return lax.rem(me + step, views)

    def row_at(step):
        return lax.rem(mr + step, rows)

    def depth_at(step):
        return lax.rem(mx + step, depths)

    def over_views(first, body):
        if views <= UNROLL:
            for step in range(first, views):
                body(step)
        else:
            pl.loop(first, views)(body)

    barrier = pltpu.get_barrier_semaphore()

    def greet(v, x, r):
        pl.semaphore_signal(
            barrier, inc=1, device_id={"view": v, "depth": x, "row": r}, device_id_type=MESH
        )

    over_views(1, lambda step: greet(view_at(step), mx, mr))
    for dx, dr in siblings:
        greet(me, depth_at(dx), row_at(dr))

    local = [
        pltpu.make_async_copy(srow.at[0], sbuf, local_sem.at[0]),
        pltpu.make_async_copy(scol.at[0], qbuf, local_sem.at[1]),
        pltpu.make_async_copy(frac.at[:, 0], wbuf, local_sem.at[2]),
        pltpu.make_async_copy(feat.at[0, pl.ds(me * cc, cc)], fbuf.at[me, mr], local_sem.at[3]),
        pltpu.make_async_copy(cot, cotv, local_sem.at[4]),
    ]
    for copy in local:
        copy.start()

    def feat_copy(step):
        to = lax.rem(me + views - step, views)
        return pltpu.make_async_remote_copy(
            src_ref=feat.at[0, pl.ds(to * cc, cc)], dst_ref=fbuf.at[me, mr],
            send_sem=f_send.at[step], recv_sem=f_recv.at[step],
            device_id={"view": to}, device_id_type=MESH,
        )

    def own_copy(dr):
        return pltpu.make_async_remote_copy(
            src_ref=feat.at[0, pl.ds(me * cc, cc)], dst_ref=fbuf.at[me, mr],
            send_sem=p_send.at[0, dr], recv_sem=p_recv.at[0, dr],
            device_id={"row": row_at(dr)}, device_id_type=MESH,
        )

    def pass_copy(step, dr):
        block = fbuf.at[view_at(step), mr]
        return pltpu.make_async_remote_copy(
            src_ref=block, dst_ref=block,
            send_sem=p_send.at[step, dr], recv_sem=p_recv.at[step, dr],
            device_id={"row": row_at(dr)}, device_id_type=MESH,
        )

    def point_copy(step):
        to = lax.rem(me + views - step, views)
        return pltpu.make_async_remote_copy(
            src_ref=cbuf.at[me], dst_ref=cbuf.at[me],
            send_sem=i_send.at[step], recv_sem=i_recv.at[step],
            device_id={"view": to}, device_id_type=MESH,
        )

    for copy in local[:3]:
        copy.wait()
    for d in range(planes):
        at = pl.ds(d * rl, rl)
        cbuf[me, 0, at, :] = sbuf[d].astype(F32) + wbuf[0, d].astype(F32) / 256.0
        cbuf[me, 1, at, :] = qbuf[d].astype(F32) + wbuf[1, d].astype(F32) / 256.0

    pl.semaphore_wait(barrier, views + len(siblings) - 1)
    for dr in range(1, rows):
        own_copy(dr).start()
    over_views(1, lambda step: feat_copy(step).start())
    over_views(1, lambda step: point_copy(step).start())

    lane = lax.broadcasted_iota(jnp.int32, (SPAN, COLS), 0).astype(F32).astype(BF16)

    def points(v):
        position = cbuf[v, 1]
        span = jnp.zeros_like(position)
        for t in range(1, spans):
            span = span + jnp.where(position >= float(t * STRIDE), 1.0, 0.0)
        inside = position - span * float(STRIDE)
        whole = jnp.floor(inside)
        return cbuf[v, 0], span, whole, inside - whole

    def row_weight(row, k, h):
        return jnp.maximum(1.0 - jnp.abs(row[k : k + 1] - float(h)), 0.0)

    def flatten(v):
        parts = []
        for h in range(height):
            line = fbuf[v, h // rl, :, h % rl, :]
            line = jnp.concatenate(
                [line, jnp.zeros((cc, (spans - 1) * STRIDE + SPAN - width), F32)], axis=1
            )
            for t in range(spans):
                parts.append(line[:, t * STRIDE : t * STRIDE + SPAN])
        flat[...] = split(jnp.concatenate(parts, axis=0), 1)

    def sampled(v, first):
        flatten(v)
        row, span, whole, rest = points(v)
        for k in range(lines):
            for n in range(0, width, COLS):
                cols = slice(n, n + COLS)
                at = jnp.broadcast_to(whole[k : k + 1, cols].astype(BF16), (SPAN, COLS))
                past = jnp.broadcast_to(rest[k : k + 1, cols].astype(BF16), (SPAN, COLS))
                mat = jnp.maximum(BF16(1.0) - jnp.abs((lane - at) - past), BF16(0.0))
                mats[v, :, k * width + n : k * width + n + COLS] = mat
                mixed = jnp.dot(
                    flat[...], jnp.concatenate([mat, mat], axis=0), preferred_element_type=F32
                )
                which = jnp.broadcast_to(span[k : k + 1, cols], (cc, COLS))
                warped = None
                for h in range(height):
                    base = h * spans * cc
                    part = mixed[base : base + cc]
                    for t in range(1, spans):
                        here = base + t * cc
                        part = jnp.where(which == float(t), mixed[here : here + cc], part)
                    part = part * row_weight(row, k, h)[:, cols]
                    warped = part if warped is None else warped + part
                warp[v, k, :, cols] = warped
                wsum[k, :, cols] = warped if first else wsum[k, :, cols] + warped

    local[4].wait()
    for k in range(lines):
        cotg[k] = factor * cotv[k // rl, :, k % rl, :]
    local[3].wait()
    for dr in range(1, rows):
        own_copy(dr).wait_recv()
    sampled(me, True)

    def pass_features(step):
        feat_copy(step).wait_recv()
        for dr in range(1, rows):
            pass_copy(step, dr).start()

    over_views(1, pass_features)

    def sample_step(step):
        point_copy(step).wait_recv()
        for dr in range(1, rows):
            pass_copy(step, dr).wait_recv()
        sampled(view_at(step), False)

    over_views(1, sample_step)

    def backward(v):
        row, span, _, _ = points(v)
        for k in range(lines):
            grad = cotg[k] * (warp[v, k] - wsum[k] / views)
            both = split(
                jnp.concatenate([grad * row_weight(row, k, h) for h in range(height)], axis=0), 0
            )
            size = 2 * height * cc
            for t in range(spans):
                mask = jnp.where(span[k : k + 1] == float(t), 1.0, 0.0).astype(BF16)
                moved[t * size : (t + 1) * size, k * width : (k + 1) * width] = both * mask
        total = lax.dot_general(
            moved[...], mats[v], (((1,), (1,)), ((), ())), preferred_element_type=F32
        )
        whole = None
        for t in range(spans):
            left = t * STRIDE
            part = total[t * size : t * size + size // 2] + total[t * size + size // 2 : (t + 1) * size]
            part = part[:, : min(SPAN, width - left)]
            right = width - left - part.shape[1]
            pieces = [jnp.zeros((size // 2, left), F32)] if left else []
            pieces.append(part)
            if right:
                pieces.append(jnp.zeros((size // 2, right), F32))
            part = jnp.concatenate(pieces, axis=1)
            whole = part if whole is None else whole + part
        for s in range(rows):
            for x in range(depths):
                for i in range(rl):
                    at = (s * rl + i) * cc
                    outbuf[v, s, x, i] = whole[at : at + cc, x * wx : (x + 1) * wx]

    def piece_copy(v, dx, dr):
        x, r = depth_at(dx), row_at(dr)
        at = dx * rows + dr
        return pltpu.make_async_remote_copy(
            src_ref=outbuf.at[v, r, x], dst_ref=pbuf.at[v, at],
            send_sem=d_send.at[v, at], recv_sem=d_recv.at[v, at],
            device_id={"depth": x, "row": r}, device_id_type=MESH,
        )

    def out_copy(step):
        v = view_at(step)
        return pltpu.make_async_remote_copy(
            src_ref=red.at[v], dst_ref=inbuf.at[me],
            send_sem=o_send.at[step], recv_sem=o_recv.at[step],
            device_id={"view": v}, device_id_type=MESH,
        )

    def add_pieces(v, target):
        piece = outbuf[v, mr, mx]
        for dx, dr in siblings:
            piece_copy(v, dx, dr).wait_recv()
            piece = piece + pbuf[v, dx * rows + dr]
        target[...] = piece

    def pass_on(step):
        v = view_at(step)
        add_pieces(v, red.at[v])
        out_copy(step).start()

    def backward_step(step):
        v = view_at(step)
        backward(v)
        for dx, dr in siblings:
            piece_copy(v, dx, dr).start()
        if views <= UNROLL:
            if step > 1:
                pass_on(step - 1)
        else:
            @pl.when(step > 1)
            def _():
                pass_on(step - 1)

    over_views(1, backward_step)
    backward(me)
    for dx, dr in siblings:
        piece_copy(me, dx, dr).start()
    if views > 1:
        pass_on(views - 1)
    add_pieces(me, inbuf.at[me])

    over_views(1, lambda step: out_copy(step).wait_recv())
    for i in range(rl):
        for u in range(views):
            out[i, pl.ds(u * cc, cc), :] = inbuf[u, i]

    for dr in range(1, rows):
        own_copy(dr).wait_send()
    for dx, dr in siblings:
        piece_copy(me, dx, dr).wait_send()

    def finish(step):
        feat_copy(step).wait_send()
        point_copy(step).wait_send()
        for dr in range(1, rows):
            pass_copy(step, dr).wait_send()
        for dx, dr in siblings:
            piece_copy(view_at(step), dx, dr).wait_send()
        out_copy(step).wait_send()

    over_views(1, finish)


def per_device(features, cotangent, src_row, src_col, fractions):
    views, depths, rows = (lax.axis_size(axis) for axis in ("view", "depth", "row"))
    channels, rl, width = features.shape[1:]
    planes, cc = cotangent.shape[:2]
    height, wx = rows * rl, width // depths
    lines = planes * rl
    spans = (width - 1) // STRIDE + 1
    sizes = (views, depths, rows, cc, planes, rl, width)
    grad = pl.pallas_call(
        functools.partial(kernel, sizes),
        out_shape=jax.ShapeDtypeStruct((rl, channels, wx), F32),
        in_specs=[pl.BlockSpec(memory_space=pl.ANY)] * 5,
        out_specs=pl.BlockSpec(memory_space=pltpu.VMEM),
        scratch_shapes=[
            pltpu.VMEM((views, rows, cc, rl, width), F32),
            pltpu.VMEM((planes, rl, width), jnp.int32),
            pltpu.VMEM((planes, rl, width), jnp.int32),
            pltpu.VMEM((2, planes, rl, width), jnp.int32),
            pltpu.VMEM((views, 2, lines, width), F32),
            pltpu.VMEM((planes, cc, rl, width), F32),
            pltpu.VMEM((lines, cc, width), F32),
            pltpu.VMEM((height * spans * cc, 2 * SPAN), BF16),
            pltpu.VMEM((views, SPAN, lines * width), BF16),
            pltpu.VMEM((2 * height * spans * cc, lines * width), BF16),
            pltpu.VMEM((views, lines, cc, width), F32),
            pltpu.VMEM((lines, cc, width), F32),
            pltpu.VMEM((views, rows, depths, rl, cc, wx), F32),
            pltpu.VMEM((views, rows * depths, rl, cc, wx), F32),
            pltpu.VMEM((views, rl, cc, wx), F32),
            pltpu.VMEM((views, rl, cc, wx), F32),
            pltpu.SemaphoreType.DMA((5,)),
            pltpu.SemaphoreType.DMA((views,)),
            pltpu.SemaphoreType.DMA((views,)),
            pltpu.SemaphoreType.DMA((views, rows)),
            pltpu.SemaphoreType.DMA((views, rows)),
            pltpu.SemaphoreType.DMA((views,)),
            pltpu.SemaphoreType.DMA((views,)),
            pltpu.SemaphoreType.DMA((views, rows * depths)),
            pltpu.SemaphoreType.DMA((views, rows * depths)),
            pltpu.SemaphoreType.DMA((views,)),
            pltpu.SemaphoreType.DMA((views,)),
        ],
        compiler_params=pltpu.CompilerParams(
            collective_id=0, has_side_effects=True, vmem_limit_bytes=60 << 20
        ),
    )(features, cotangent, src_row, src_col, fractions)
    return jnp.transpose(grad, (1, 0, 2))[None]


def solution(mesh):
    in_specs = (
        P("view", None, ("group", "row"), None),
        P("depth", "view", ("group", "row"), None),
        P("view", "depth", ("group", "row"), None),
        P("view", "depth", ("group", "row"), None),
        P(None, "view", "depth", ("group", "row"), None),
    )
    out_specs = P("view", None, ("group", "row"), "depth")
    return jax.shard_map(
        per_device, mesh=mesh, in_specs=in_specs, out_specs=out_specs, check_vma=False
    )
```

```python
import functools

import jax
import jax.numpy as jnp
from jax import lax
from jax.experimental import pallas as pl
from jax.experimental.pallas import tpu as pltpu
from jax.sharding import PartitionSpec as P

MESH = pl.DeviceIdType.MESH
F32 = jnp.float32
BF16 = jnp.bfloat16
SPAN = 128
STRIDE = SPAN - 1
COLS = 256
UNROLL = 4


def split(value, axis):
    high = value.astype(BF16)
    low = (value - high.astype(F32)).astype(BF16)
    return jnp.concatenate([high, low], axis=axis)


def kernel(
    sizes, feat, cot, srow, scol, frac, out,
    fbuf, sbuf, qbuf, wbuf, cbuf, cotv, cotg, flat, mats, moved, warp, wsum, outbuf, pbuf, red,
    local_sem, f_send, f_recv, p_send, p_recv, i_send, i_recv, d_send, d_recv, o_send, o_recv,
):
    views, depths, rows, cc, planes, rl, width = sizes
    me = lax.axis_index("view")
    mx = lax.axis_index("depth")
    mr = lax.axis_index("row")
    height = rows * rl
    wx = width // depths
    lines = planes * rl
    spans = (width - 1) // STRIDE + 1
    factor = 2.0 / views
    siblings = [(dx, dr) for dx in range(depths) for dr in range(rows) if dx or dr]

    def row_at(step):
        return lax.rem(mr + step, rows)

    def depth_at(step):
        return lax.rem(mx + step, depths)

    def others(body):
        if views <= UNROLL:
            for at in range(1, views):
                body(views - at)
        else:
            pl.loop(1, views)(lambda at: body(views - at))

    def paired(step):
        if views & (views - 1):
            return lax.rem(views - me + step, views)
        other, bit = 0, 1
        while bit < views:
            other = other + bit * lax.rem(me // bit + step // bit, 2)
            bit *= 2
        return other

    barrier = pltpu.get_barrier_semaphore()

    def greet(v, x, r):
        pl.semaphore_signal(
            barrier, inc=1, device_id={"view": v, "depth": x, "row": r}, device_id_type=MESH
        )

    others(lambda step: greet(paired(step), mx, mr))
    for dx, dr in siblings:
        greet(me, depth_at(dx), row_at(dr))

    local = [
        pltpu.make_async_copy(srow.at[0], sbuf, local_sem.at[0]),
        pltpu.make_async_copy(scol.at[0], qbuf, local_sem.at[1]),
        pltpu.make_async_copy(frac.at[:, 0], wbuf, local_sem.at[2]),
        pltpu.make_async_copy(feat.at[0, pl.ds(me * cc, cc)], fbuf.at[me, mr], local_sem.at[3]),
        pltpu.make_async_copy(cot, cotv, local_sem.at[4]),
    ]
    for copy in local:
        copy.start()

    mine = pl.ds(pl.multiple_of(mx * wx, SPAN), wx)

    def feat_copy(step):
        to = paired(step)
        return pltpu.make_async_remote_copy(
            src_ref=feat.at[0, pl.ds(to * cc, cc), :, mine], dst_ref=fbuf.at[me, mr, :, :, mine],
            send_sem=f_send.at[step], recv_sem=f_recv.at[step],
            device_id={"view": to}, device_id_type=MESH,
        )

    def own_copy(dr):
        return pltpu.make_async_remote_copy(
            src_ref=feat.at[0, pl.ds(me * cc, cc)], dst_ref=fbuf.at[me, mr],
            send_sem=p_send.at[0, dr], recv_sem=p_recv.at[0, dr],
            device_id={"row": row_at(dr)}, device_id_type=MESH,
        )

    def pass_copies(step):
        block = fbuf.at[paired(step), mr, :, :, mine]
        return [
            pltpu.make_async_remote_copy(
                src_ref=block, dst_ref=block,
                send_sem=p_send.at[step, dx * rows + dr], recv_sem=p_recv.at[step, dx * rows + dr],
                device_id={"depth": depth_at(dx), "row": row_at(dr)}, device_id_type=MESH,
            )
            for dx, dr in siblings
        ]

    def point_copy(step):
        return pltpu.make_async_remote_copy(
            src_ref=cbuf.at[me], dst_ref=cbuf.at[me],
            send_sem=i_send.at[step], recv_sem=i_recv.at[step],
            device_id={"view": paired(step)}, device_id_type=MESH,
        )

    pl.semaphore_wait(barrier, views + len(siblings) - 1)
    for dr in range(1, rows):
        own_copy(dr).start()
    others(lambda step: feat_copy(step).start())

    for copy in local[:3]:
        copy.wait()
    for d in range(planes):
        at = pl.ds(d * rl, rl)
        cbuf[me, 0, at, :] = sbuf[d].astype(F32) + wbuf[0, d].astype(F32) / 256.0
        cbuf[me, 1, at, :] = qbuf[d].astype(F32) + wbuf[1, d].astype(F32) / 256.0

    others(lambda step: point_copy(step).start())

    lane = lax.broadcasted_iota(jnp.int32, (SPAN, COLS), 0).astype(F32).astype(BF16)

    def points(v):
        position = cbuf[v, 1]
        span = jnp.zeros_like(position)
        for t in range(1, spans):
            span = span + jnp.where(position >= float(t * STRIDE), 1.0, 0.0)
        inside = position - span * float(STRIDE)
        whole = jnp.floor(inside)
        return cbuf[v, 0], span, whole, inside - whole

    def row_weight(row, k, h):
        return jnp.maximum(1.0 - jnp.abs(row[k : k + 1] - float(h)), 0.0)

    def flatten(v):
        parts = []
        for h in range(height):
            line = fbuf[v, h // rl, :, h % rl, :]
            line = jnp.concatenate(
                [line, jnp.zeros((cc, (spans - 1) * STRIDE + SPAN - width), F32)], axis=1
            )
            for t in range(spans):
                parts.append(line[:, t * STRIDE : t * STRIDE + SPAN])
        flat[...] = split(jnp.concatenate(parts, axis=0), 1)

    def sampled(v, first):
        flatten(v)
        row, span, whole, rest = points(v)
        for k in range(lines):
            for n in range(0, width, COLS):
                cols = slice(n, n + COLS)
                at = jnp.broadcast_to(whole[k : k + 1, cols].astype(BF16), (SPAN, COLS))
                past = jnp.broadcast_to(rest[k : k + 1, cols].astype(BF16), (SPAN, COLS))
                mat = jnp.maximum(BF16(1.0) - jnp.abs((lane - at) - past), BF16(0.0))
                mats[v, :, k * width + n : k * width + n + COLS] = mat
                mixed = jnp.dot(
                    flat[...], jnp.concatenate([mat, mat], axis=0), preferred_element_type=F32
                )
                which = jnp.broadcast_to(span[k : k + 1, cols], (cc, COLS))
                warped = None
                for h in range(height):
                    base = h * spans * cc
                    part = mixed[base : base + cc]
                    for t in range(1, spans):
                        here = base + t * cc
                        part = jnp.where(which == float(t), mixed[here : here + cc], part)
                    part = part * row_weight(row, k, h)[:, cols]
                    warped = part if warped is None else warped + part
                warp[v, k, :, cols] = warped
                wsum[k, :, cols] = warped if first else wsum[k, :, cols] + warped

    local[4].wait()
    for k in range(lines):
        cotg[k] = factor * cotv[k // rl, :, k % rl, :]
    local[3].wait()
    for dr in range(1, rows):
        own_copy(dr).wait_recv()
    sampled(me, True)

    def pass_features(step):
        feat_copy(step).wait_recv()
        for copy in pass_copies(step):
            copy.start()

    others(pass_features)

    def sample_step(step):
        point_copy(step).wait_recv()
        for copy in pass_copies(step):
            copy.wait_recv()
        sampled(paired(step), False)

    others(sample_step)

    def backward(v):
        row, span, _, _ = points(v)
        for k in range(lines):
            grad = cotg[k] * (warp[v, k] - wsum[k] / views)
            both = split(
                jnp.concatenate([grad * row_weight(row, k, h) for h in range(height)], axis=0), 0
            )
            size = 2 * height * cc
            for t in range(spans):
                mask = jnp.where(span[k : k + 1] == float(t), 1.0, 0.0).astype(BF16)
                moved[t * size : (t + 1) * size, k * width : (k + 1) * width] = both * mask
        total = lax.dot_general(
            moved[...], mats[v], (((1,), (1,)), ((), ())), preferred_element_type=F32
        )
        whole = None
        for t in range(spans):
            left = t * STRIDE
            part = total[t * size : t * size + size // 2] + total[t * size + size // 2 : (t + 1) * size]
            part = part[:, : min(SPAN, width - left)]
            right = width - left - part.shape[1]
            pieces = [jnp.zeros((size // 2, left), F32)] if left else []
            pieces.append(part)
            if right:
                pieces.append(jnp.zeros((size // 2, right), F32))
            part = jnp.concatenate(pieces, axis=1)
            whole = part if whole is None else whole + part
        for s in range(rows):
            for x in range(depths):
                for i in range(rl):
                    at = (s * rl + i) * cc
                    outbuf[v, s, x, :, i, :] = whole[at : at + cc, x * wx : (x + 1) * wx]

    def piece_copy(v, dx, dr):
        x, r = depth_at(dx), row_at(dr)
        at = dx * rows + dr
        return pltpu.make_async_remote_copy(
            src_ref=outbuf.at[v, r, x], dst_ref=pbuf.at[v, at],
            send_sem=d_send.at[v, at], recv_sem=d_recv.at[v, at],
            device_id={"depth": x, "row": r}, device_id_type=MESH,
        )

    def out_copy(step):
        v = paired(step)
        return pltpu.make_async_remote_copy(
            src_ref=red.at[v], dst_ref=out.at[pl.ds(me * cc, cc)],
            send_sem=o_send.at[step], recv_sem=o_recv.at[step],
            device_id={"view": v}, device_id_type=MESH,
        )

    def add_pieces(v):
        piece = outbuf[v, mr, mx]
        for dx, dr in siblings:
            piece_copy(v, dx, dr).wait_recv()
            piece = piece + pbuf[v, dx * rows + dr]
        return piece

    def pass_on(step):
        v = paired(step)
        red[v] = add_pieces(v)
        out_copy(step).start()

    def backward_step(step):
        v = paired(step)
        backward(v)
        for dx, dr in siblings:
            piece_copy(v, dx, dr).start()
    pl.loop(1, views)(lambda at: backward_step(views - at))
    backward(me)
    for dx, dr in siblings:
        piece_copy(me, dx, dr).start()
    others(pass_on)
    out[pl.ds(me * cc, cc)] = add_pieces(me)

    others(lambda step: out_copy(step).wait_recv())

    for dr in range(1, rows):
        own_copy(dr).wait_send()
    for dx, dr in siblings:
        piece_copy(me, dx, dr).wait_send()

    def finish(step):
        feat_copy(step).wait_send()
        point_copy(step).wait_send()
        for copy in pass_copies(step):
            copy.wait_send()
        for dx, dr in siblings:
            piece_copy(paired(step), dx, dr).wait_send()
        out_copy(step).wait_send()

    others(finish)


def per_device(features, cotangent, src_row, src_col, fractions):
    views, depths, rows = (lax.axis_size(axis) for axis in ("view", "depth", "row"))
    channels, rl, width = features.shape[1:]
    planes, cc = cotangent.shape[:2]
    height, wx = rows * rl, width // depths
    lines = planes * rl
    spans = (width - 1) // STRIDE + 1
    sizes = (views, depths, rows, cc, planes, rl, width)
    grad = pl.pallas_call(
        functools.partial(kernel, sizes),
        out_shape=pltpu.VMEM((channels, rl, wx), F32),
        in_specs=[pl.BlockSpec(memory_space=pl.ANY)] * 5,
        out_specs=pl.BlockSpec(memory_space=pltpu.VMEM),
        scratch_shapes=[
            pltpu.VMEM((views, rows, cc, rl, width), F32),
            pltpu.VMEM((planes, rl, width), jnp.int32),
            pltpu.VMEM((planes, rl, width), jnp.int32),
            pltpu.VMEM((2, planes, rl, width), jnp.int32),
            pltpu.VMEM((views, 2, lines, width), F32),
            pltpu.VMEM((planes, cc, rl, width), F32),
            pltpu.VMEM((lines, cc, width), F32),
            pltpu.VMEM((height * spans * cc, 2 * SPAN), BF16),
            pltpu.VMEM((views, SPAN, lines * width), BF16),
            pltpu.VMEM((2 * height * spans * cc, lines * width), BF16),
            pltpu.VMEM((views, lines, cc, width), F32),
            pltpu.VMEM((lines, cc, width), F32),
            pltpu.VMEM((views, rows, depths, cc, rl, wx), F32),
            pltpu.VMEM((views, rows * depths, cc, rl, wx), F32),
            pltpu.VMEM((views, cc, rl, wx), F32),
            pltpu.SemaphoreType.DMA((5,)),
            pltpu.SemaphoreType.DMA((views,)),
            pltpu.SemaphoreType.DMA((views,)),
            pltpu.SemaphoreType.DMA((views, rows * depths)),
            pltpu.SemaphoreType.DMA((views, rows * depths)),
            pltpu.SemaphoreType.DMA((views,)),
            pltpu.SemaphoreType.DMA((views,)),
            pltpu.SemaphoreType.DMA((views, rows * depths)),
            pltpu.SemaphoreType.DMA((views, rows * depths)),
            pltpu.SemaphoreType.DMA((views,)),
            pltpu.SemaphoreType.DMA((views,)),
        ],
        compiler_params=pltpu.CompilerParams(
            collective_id=0, has_side_effects=True, vmem_limit_bytes=60 << 20
        ),
    )(features, cotangent, src_row, src_col, fractions)
    return grad[None]


def solution(mesh):
    in_specs = (
        P("view", None, ("group", "row"), None),
        P("depth", "view", ("group", "row"), None),
        P("view", "depth", ("group", "row"), None),
        P("view", "depth", ("group", "row"), None),
        P(None, "view", "depth", ("group", "row"), None),
    )
    out_specs = P("view", None, ("group", "row"), "depth")
    return jax.shard_map(
        per_device, mesh=mesh, in_specs=in_specs, out_specs=out_specs, check_vma=False
    )
```

```python
import functools

import jax
import jax.numpy as jnp
from jax import lax
from jax.experimental import pallas as pl
from jax.experimental.pallas import tpu as pltpu
from jax.sharding import PartitionSpec as P

MESH = pl.DeviceIdType.MESH
F32 = jnp.float32
BF16 = jnp.bfloat16
SPAN = 128
COLS = 256
UNROLL = 4


def split(value, axis):
    high = value.astype(BF16)
    low = (value - high.astype(F32)).astype(BF16)
    return jnp.concatenate([high, low], axis=axis)


def kernel(
    sizes, feat, cot, srow, scol, frac, out,
    fbuf, sbuf, qbuf, wbuf, cbuf, cotv, cotg, flat, edge, mats, moved, warp, wsum, outbuf, pbuf, red, inbuf,
    local_sem, f_send, f_recv, p_send, p_recv, i_send, i_recv, d_send, d_recv, o_send, o_recv,
):
    views, depths, rows, cc, planes, rl, width = sizes
    me = lax.axis_index("view")
    mx = lax.axis_index("depth")
    mr = lax.axis_index("row")
    height = rows * rl
    wx = width // depths
    lines = planes * rl
    spans = width // SPAN
    half = height * cc
    factor = 2.0 / views
    siblings = [(dx, dr) for dx in range(depths) for dr in range(rows) if dx or dr]

    def row_at(step):
        return lax.rem(mr + step, rows)

    def depth_at(step):
        return lax.rem(mx + step, depths)

    def step_of(at):
        return (views // 2 + at - 2) % (views - 1) + 1

    steps = [step_of(at) for at in range(1, views)]

    def paired(step):
        other, bit = 0, 1
        while bit < views:
            other = other + bit * lax.rem(me // bit + step // bit, 2)
            bit *= 2
        return other

    def lowest(step):
        return step & -step

    barrier = pltpu.get_barrier_semaphore()

    def greet(v, x, r):
        pl.semaphore_signal(
            barrier, inc=1, device_id={"view": v, "depth": x, "row": r}, device_id_type=MESH
        )

    for step in steps:
        greet(paired(step), mx, mr)
    for dx in range(1, depths):
        for step in steps:
            greet(paired(step), depth_at(dx), mr)
        greet(me, depth_at(dx), mr)
    for dr in range(1, rows):
        greet(me, mx, row_at(dr))

    local = [
        pltpu.make_async_copy(srow.at[0], sbuf, local_sem.at[0]),
        pltpu.make_async_copy(scol.at[0], qbuf, local_sem.at[1]),
        pltpu.make_async_copy(frac.at[:, 0], wbuf, local_sem.at[2]),
        pltpu.make_async_copy(feat.at[0, pl.ds(me * cc, cc)], fbuf.at[me, mr], local_sem.at[3]),
        pltpu.make_async_copy(cot, cotv, local_sem.at[4]),
    ]
    for copy in local:
        copy.start()

    def feat_copy(step):
        to = paired(step)
        return pltpu.make_async_remote_copy(
            src_ref=feat.at[0, pl.ds(to * cc, cc)], dst_ref=fbuf.at[me, mr],
            send_sem=f_send.at[step], recv_sem=f_recv.at[step],
            device_id={"view": to}, device_id_type=MESH,
        )

    def own_copy(dr):
        return pltpu.make_async_remote_copy(
            src_ref=feat.at[0, pl.ds(me * cc, cc)], dst_ref=fbuf.at[me, mr],
            send_sem=p_send.at[0, dr], recv_sem=p_recv.at[0, dr],
            device_id={"row": row_at(dr)}, device_id_type=MESH,
        )

    def pass_copies(step):
        block = fbuf.at[paired(step), mr]
        return [
            pltpu.make_async_remote_copy(
                src_ref=block, dst_ref=block,
                send_sem=p_send.at[step, dr], recv_sem=p_recv.at[step, dr],
                device_id={"row": row_at(dr)}, device_id_type=MESH,
            )
            for dr in range(1, rows)
        ]

    def point_copy(step):
        block = cbuf.at[paired(step - lowest(step))]
        return pltpu.make_async_remote_copy(
            src_ref=block, dst_ref=block,
            send_sem=i_send.at[step], recv_sem=i_recv.at[step],
            device_id={"view": paired(lowest(step))}, device_id_type=MESH,
        )

    for copy in local[:3]:
        copy.wait()
    for d in range(planes):
        at = pl.ds(d * rl, rl)
        cbuf[me, 0, at, :] = sbuf[d].astype(F32) + wbuf[0, d].astype(F32) / 256.0
        cbuf[me, 1, at, :] = qbuf[d].astype(F32) + wbuf[1, d].astype(F32) / 256.0

    pl.semaphore_wait(barrier, views * depths + rows - 2)
    own_points = [step for step in steps if step == lowest(step)]
    for step in own_points:
        point_copy(step).start()
    for dr in range(1, rows):
        own_copy(dr).start()
    for step in steps:
        feat_copy(step).start()

    lane = lax.broadcasted_iota(jnp.int32, (SPAN, COLS), 0).astype(F32).astype(BF16)

    def points(v):
        position = cbuf[v, 1]
        span = jnp.zeros_like(position)
        for t in range(1, spans):
            span = span + jnp.where(position >= float(t * SPAN), 1.0, 0.0)
        inside = position - span * float(SPAN)
        whole = jnp.floor(inside)
        rest = inside - whole
        return cbuf[v, 0], span, whole, rest, jnp.where(whole == float(SPAN - 1), rest, 0.0)

    def row_weight(row, k, h):
        return jnp.maximum(1.0 - jnp.abs(row[k : k + 1] - float(h)), 0.0)

    def flatten(v):
        parts = []
        for h in range(height):
            line = fbuf[v, h // rl, :, h % rl, :]
            for t in range(spans):
                parts.append(line[:, t * SPAN : (t + 1) * SPAN])
                if t:
                    first = line[:, t * SPAN : t * SPAN + 1]
                    edge[h, t - 1] = jnp.broadcast_to(first, (cc, COLS))
        flat[...] = split(jnp.concatenate(parts, axis=0), 1)

    def sampled(v, first):
        flatten(v)
        row, span, whole, rest, over = points(v)
        for k in range(lines):
            for n in range(0, width, COLS):
                cols = slice(n, n + COLS)
                at = jnp.broadcast_to(whole[k : k + 1, cols].astype(BF16), (SPAN, COLS))
                past = jnp.broadcast_to(rest[k : k + 1, cols].astype(BF16), (SPAN, COLS))
                mat = jnp.maximum(BF16(1.0) - jnp.abs((lane - at) - past), BF16(0.0))
                mats[v, :, k * width + n : k * width + n + COLS] = mat
                mixed = jnp.dot(
                    flat[...], jnp.concatenate([mat, mat], axis=0), preferred_element_type=F32
                )
                which = jnp.broadcast_to(span[k : k + 1, cols], (cc, COLS))
                beyond = jnp.broadcast_to(over[k : k + 1, cols], (cc, COLS))
                warped = None
                for h in range(height):
                    base = h * spans * cc
                    part, tail = mixed[base : base + cc], edge[h, 0] if spans > 1 else None
                    for t in range(1, spans):
                        here = base + t * cc
                        inside = which == float(t)
                        part = jnp.where(inside, mixed[here : here + cc], part)
                        if t < spans - 1:
                            tail = jnp.where(inside, edge[h, t], tail)
                    if tail is not None:
                        part = part + beyond * tail
                    part = part * row_weight(row, k, h)[:, cols]
                    warped = part if warped is None else warped + part
                warp[v, k, :, cols] = warped
                wsum[k, :, cols] = warped if first else wsum[k, :, cols] + warped

    local[4].wait()
    for k in range(lines):
        cotg[k] = factor * cotv[k // rl, :, k % rl, :]
    local[3].wait()
    for dr in range(1, rows):
        own_copy(dr).wait_recv()
    sampled(me, True)

    bit = views // 4
    while bit:
        for step in steps:
            if lowest(step) == 2 * bit:
                point_copy(step).wait_recv()
        for step in steps:
            if lowest(step) == bit and step != bit:
                point_copy(step).start()
        bit //= 2

    for step in sorted(steps):
        feat_copy(step).wait_recv()
        for copy in pass_copies(step):
            copy.start()

    def ready(step):
        if lowest(step) == 1:
            point_copy(step).wait_recv()
        for copy in pass_copies(step):
            copy.wait_recv()

    if views <= UNROLL:
        for step in sorted(steps):
            ready(step)
            sampled(paired(step), False)
    else:
        for step in steps:
            ready(step)
        pl.loop(1, views)(lambda step: sampled(paired(step), False))

    def backward(v):
        row, span, _, _, over = points(v)
        size = 2 * half
        crossing = [jnp.zeros((half, SPAN), F32)] * (spans - 1)
        for k in range(lines):
            grad = cotg[k] * (warp[v, k] - wsum[k] / views)
            spread = jnp.concatenate([grad * row_weight(row, k, h) for h in range(height)], axis=0)
            both = split(spread, 0)
            for t in range(spans):
                mask = jnp.where(span[k : k + 1] == float(t), 1.0, 0.0)
                moved[t * size : (t + 1) * size, k * width : (k + 1) * width] = both * mask.astype(BF16)
                if t < spans - 1:
                    beyond = spread * (mask * over[k : k + 1])
                    for n in range(0, width, SPAN):
                        crossing[t] = crossing[t] + beyond[:, n : n + SPAN]
        total = lax.dot_general(
            moved[...], mats[v], (((1,), (1,)), ((), ())), preferred_element_type=F32
        )
        starts = lax.broadcasted_iota(jnp.int32, (half, SPAN), 1) == 0
        for t in range(spans):
            part = total[t * size : t * size + half] + total[t * size + half : (t + 1) * size]
            if t:
                part = part + jnp.where(starts, jnp.sum(crossing[t - 1], axis=1, keepdims=True), 0.0)
            x, left = t * SPAN // wx, t * SPAN % wx
            for s in range(rows):
                for i in range(rl):
                    at = (s * rl + i) * cc
                    outbuf[v, s, x, :, i, left : left + SPAN] = part[at : at + cc]

    def core_copy(v, dr):
        r = row_at(dr)
        return pltpu.make_async_remote_copy(
            src_ref=outbuf.at[v, r], dst_ref=pbuf.at[v, dr],
            send_sem=d_send.at[v, dr], recv_sem=d_recv.at[v, dr],
            device_id={"row": r}, device_id_type=MESH,
        )

    def out_copy(v, step, dx):
        x = depth_at(dx)
        return pltpu.make_async_remote_copy(
            src_ref=red.at[v, x], dst_ref=inbuf.at[me, mx],
            send_sem=o_send.at[step, dx], recv_sem=o_recv.at[step, dx],
            device_id={"view": v, "depth": x}, device_id_type=MESH,
        )

    def add_cores(v):
        piece = outbuf[v, mr]
        for dr in range(1, rows):
            core_copy(v, dr).wait_recv()
            piece = piece + pbuf[v, dr]
        red[v] = piece

    def other_at(at):
        return at - 1 + (at - 1 + views - me) // views

    def pass_on(v):
        add_cores(v)
        for dx in range(depths):
            out_copy(v, paired(v), dx).start()

    @pl.loop(1, views)
    def _(at):
        v = other_at(at)
        backward(v)
        for dr in range(1, rows):
            core_copy(v, dr).start()

        @pl.when(at > 1)
        def _():
            pass_on(other_at(at - 1))

    backward(me)
    for dr in range(1, rows):
        core_copy(me, dr).start()
    if views > 1:
        pass_on(other_at(views - 1))
    add_cores(me)
    for dx in range(1, depths):
        out_copy(me, 0, dx).start()
    inbuf[me, mx] = red[me, mx]

    def arrived(step):
        for dx in range(depths):
            out_copy(paired(step), step, dx).wait_recv()

    for step in steps:
        arrived(step)
    for dx in range(1, depths):
        out_copy(me, 0, dx).wait_recv()
    for u in range(views):
        piece = inbuf[u, 0]
        for x in range(1, depths):
            piece = piece + inbuf[u, x]
        out[u * cc : (u + 1) * cc] = piece

    for dr in range(1, rows):
        own_copy(dr).wait_send()
        core_copy(me, dr).wait_send()
    for dx in range(1, depths):
        out_copy(me, 0, dx).wait_send()

    def finish(step):
        feat_copy(step).wait_send()
        point_copy(step).wait_send()
        for copy in pass_copies(step):
            copy.wait_send()
        for dr in range(1, rows):
            core_copy(paired(step), dr).wait_send()
        for dx in range(depths):
            out_copy(paired(step), step, dx).wait_send()

    for step in steps:
        finish(step)


def per_device(features, cotangent, src_row, src_col, fractions):
    views, depths, rows = (lax.axis_size(axis) for axis in ("view", "depth", "row"))
    channels, rl, width = features.shape[1:]
    planes, cc = cotangent.shape[:2]
    height, wx = rows * rl, width // depths
    lines = planes * rl
    spans = width // SPAN
    sizes = (views, depths, rows, cc, planes, rl, width)
    grad = pl.pallas_call(
        functools.partial(kernel, sizes),
        out_shape=pltpu.VMEM((channels, rl, wx), F32),
        in_specs=[pl.BlockSpec(memory_space=pl.ANY)] * 5,
        out_specs=pl.BlockSpec(memory_space=pltpu.VMEM),
        scratch_shapes=[
            pltpu.VMEM((views, rows, cc, rl, width), F32),
            pltpu.VMEM((planes, rl, width), jnp.int32),
            pltpu.VMEM((planes, rl, width), jnp.int32),
            pltpu.VMEM((2, planes, rl, width), jnp.int32),
            pltpu.VMEM((views, 2, lines, width), F32),
            pltpu.VMEM((planes, cc, rl, width), F32),
            pltpu.VMEM((lines, cc, width), F32),
            pltpu.VMEM((height * spans * cc, 2 * SPAN), BF16),
            pltpu.VMEM((height, max(spans - 1, 1), cc, COLS), F32),
            pltpu.VMEM((views, SPAN, lines * width), BF16),
            pltpu.VMEM((2 * height * spans * cc, lines * width), BF16),
            pltpu.VMEM((views, lines, cc, width), F32),
            pltpu.VMEM((lines, cc, width), F32),
            pltpu.VMEM((views, rows, depths, cc, rl, wx), F32),
            pltpu.VMEM((views, rows, depths, cc, rl, wx), F32),
            pltpu.VMEM((views, depths, cc, rl, wx), F32),
            pltpu.VMEM((views, depths, cc, rl, wx), F32),
            pltpu.SemaphoreType.DMA((5,)),
            pltpu.SemaphoreType.DMA((views,)),
            pltpu.SemaphoreType.DMA((views,)),
            pltpu.SemaphoreType.DMA((views, rows)),
            pltpu.SemaphoreType.DMA((views, rows)),
            pltpu.SemaphoreType.DMA((views,)),
            pltpu.SemaphoreType.DMA((views,)),
            pltpu.SemaphoreType.DMA((views, rows)),
            pltpu.SemaphoreType.DMA((views, rows)),
            pltpu.SemaphoreType.DMA((views, depths)),
            pltpu.SemaphoreType.DMA((views, depths)),
        ],
        compiler_params=pltpu.CompilerParams(
            collective_id=0, has_side_effects=True, vmem_limit_bytes=60 << 20
        ),
    )(features, cotangent, src_row, src_col, fractions)
    return grad[None]


def solution(mesh):
    in_specs = (
        P("view", None, ("group", "row"), None),
        P("depth", "view", ("group", "row"), None),
        P("view", "depth", ("group", "row"), None),
        P("view", "depth", ("group", "row"), None),
        P(None, "view", "depth", ("group", "row"), None),
    )
    out_specs = P("view", None, ("group", "row"), "depth")
    return jax.shard_map(
        per_device, mesh=mesh, in_specs=in_specs, out_specs=out_specs, check_vma=False
    )
```

```python
import functools

import jax
import jax.numpy as jnp
from jax import lax
from jax.experimental import pallas as pl
from jax.experimental.pallas import tpu as pltpu
from jax.sharding import PartitionSpec as P

MESH = pl.DeviceIdType.MESH
F32 = jnp.float32
BF16 = jnp.bfloat16
SPAN = 128
COLS = 256
UNROLL = 4


def split(value, axis):
    high = value.astype(BF16)
    low = (value - high.astype(F32)).astype(BF16)
    return jnp.concatenate([high, low], axis=axis)


def kernel(
    sizes, feat, cot, srow, scol, frac, out,
    fbuf, sbuf, qbuf, wbuf, cbuf, cotv, cotg, flat, edge, mats, moved, warp, wsum, outbuf, pbuf, red, inbuf,
    local_sem, f_send, f_recv, p_send, p_recv, i_send, i_recv, d_send, d_recv, o_send, o_recv,
):
    views, depths, rows, cc, planes, rl, width = sizes
    me = lax.axis_index("view")
    mx = lax.axis_index("depth")
    mr = lax.axis_index("row")
    height = rows * rl
    wx = width // depths
    lines = planes * rl
    spans = width // SPAN
    half = height * cc
    factor = 2.0 / views
    siblings = [(dx, dr) for dx in range(depths) for dr in range(rows) if dx or dr]

    def row_at(step):
        return lax.rem(mr + step, rows)

    def depth_at(step):
        return lax.rem(mx + step, depths)

    def step_of(at):
        return views - at

    steps = [step_of(at) for at in range(1, views)]

    def paired(step):
        other, bit = 0, 1
        while bit < views:
            other = other + bit * lax.rem(me // bit + step // bit, 2)
            bit *= 2
        return other

    def lowest(step):
        return step & -step

    barrier = pltpu.get_barrier_semaphore()

    def greet(v, x, r):
        pl.semaphore_signal(
            barrier, inc=1, device_id={"view": v, "depth": x, "row": r}, device_id_type=MESH
        )

    for step in steps:
        greet(paired(step), mx, mr)
    for dx in range(1, depths):
        for step in steps:
            greet(paired(step), depth_at(dx), mr)
        greet(me, depth_at(dx), mr)
    for dr in range(1, rows):
        greet(me, mx, row_at(dr))

    local = [
        pltpu.make_async_copy(srow.at[0], sbuf, local_sem.at[0]),
        pltpu.make_async_copy(scol.at[0], qbuf, local_sem.at[1]),
        pltpu.make_async_copy(frac.at[:, 0], wbuf, local_sem.at[2]),
        pltpu.make_async_copy(feat.at[0, pl.ds(me * cc, cc)], fbuf.at[me, mr], local_sem.at[3]),
        pltpu.make_async_copy(cot, cotv, local_sem.at[4]),
    ]
    for copy in local:
        copy.start()

    def feat_copy(step):
        to = paired(step)
        return pltpu.make_async_remote_copy(
            src_ref=feat.at[0, pl.ds(to * cc, cc)], dst_ref=fbuf.at[me, mr],
            send_sem=f_send.at[step], recv_sem=f_recv.at[step],
            device_id={"view": to}, device_id_type=MESH,
        )

    def own_copy(dr):
        return pltpu.make_async_remote_copy(
            src_ref=feat.at[0, pl.ds(me * cc, cc)], dst_ref=fbuf.at[me, mr],
            send_sem=p_send.at[0, dr], recv_sem=p_recv.at[0, dr],
            device_id={"row": row_at(dr)}, device_id_type=MESH,
        )

    def pass_copies(step):
        block = fbuf.at[paired(step), mr]
        return [
            pltpu.make_async_remote_copy(
                src_ref=block, dst_ref=block,
                send_sem=p_send.at[step, dr], recv_sem=p_recv.at[step, dr],
                device_id={"row": row_at(dr)}, device_id_type=MESH,
            )
            for dr in range(1, rows)
        ]

    def point_copy(step):
        block = cbuf.at[paired(step - lowest(step))]
        return pltpu.make_async_remote_copy(
            src_ref=block, dst_ref=block,
            send_sem=i_send.at[step], recv_sem=i_recv.at[step],
            device_id={"view": paired(lowest(step))}, device_id_type=MESH,
        )

    for copy in local[:3]:
        copy.wait()
    for d in range(planes):
        at = pl.ds(d * rl, rl)
        cbuf[me, 0, at, :] = sbuf[d].astype(F32) + wbuf[0, d].astype(F32) / 256.0
        cbuf[me, 1, at, :] = qbuf[d].astype(F32) + wbuf[1, d].astype(F32) / 256.0

    pl.semaphore_wait(barrier, views * depths + rows - 2)
    own_points = [step for step in steps if step == lowest(step)]
    for step in own_points:
        point_copy(step).start()
    for dr in range(1, rows):
        own_copy(dr).start()
    for step in range(1, views):
        feat_copy(step).start()

    lane = lax.broadcasted_iota(jnp.int32, (SPAN, COLS), 0).astype(F32).astype(BF16)

    def points(v):
        position = cbuf[v, 1]
        span = jnp.zeros_like(position)
        for t in range(1, spans):
            span = span + jnp.where(position >= float(t * SPAN), 1.0, 0.0)
        inside = position - span * float(SPAN)
        whole = jnp.floor(inside)
        rest = inside - whole
        return cbuf[v, 0], span, whole, rest, jnp.where(whole == float(SPAN - 1), rest, 0.0)

    def row_weight(row, k, h):
        return jnp.maximum(1.0 - jnp.abs(row[k : k + 1] - float(h)), 0.0)

    def flatten(v):
        parts = []
        for h in range(height):
            line = fbuf[v, h // rl, :, h % rl, :]
            for t in range(spans):
                parts.append(line[:, t * SPAN : (t + 1) * SPAN])
                if t:
                    first = line[:, t * SPAN : t * SPAN + 1]
                    edge[h, t - 1] = jnp.broadcast_to(first, (cc, COLS))
        flat[...] = split(jnp.concatenate(parts, axis=0), 1)

    def sampled(v, first):
        flatten(v)
        row, span, whole, rest, over = points(v)
        for k in range(lines):
            for n in range(0, width, COLS):
                cols = slice(n, n + COLS)
                at = jnp.broadcast_to(whole[k : k + 1, cols].astype(BF16), (SPAN, COLS))
                past = jnp.broadcast_to(rest[k : k + 1, cols].astype(BF16), (SPAN, COLS))
                mat = jnp.maximum(BF16(1.0) - jnp.abs((lane - at) - past), BF16(0.0))
                mats[v, :, k * width + n : k * width + n + COLS] = mat
                mixed = jnp.dot(
                    flat[...], jnp.concatenate([mat, mat], axis=0), preferred_element_type=F32
                )
                which = jnp.broadcast_to(span[k : k + 1, cols], (cc, COLS))
                beyond = jnp.broadcast_to(over[k : k + 1, cols], (cc, COLS))
                warped = None
                for h in range(height):
                    base = h * spans * cc
                    part, tail = mixed[base : base + cc], edge[h, 0] if spans > 1 else None
                    for t in range(1, spans):
                        here = base + t * cc
                        inside = which == float(t)
                        part = jnp.where(inside, mixed[here : here + cc], part)
                        if t < spans - 1:
                            tail = jnp.where(inside, edge[h, t], tail)
                    if tail is not None:
                        part = part + beyond * tail
                    part = part * row_weight(row, k, h)[:, cols]
                    warped = part if warped is None else warped + part
                warp[v, k, :, cols] = warped
                wsum[k, :, cols] = warped if first else wsum[k, :, cols] + warped

    local[4].wait()
    for k in range(lines):
        cotg[k] = factor * cotv[k // rl, :, k % rl, :]
    local[3].wait()
    for dr in range(1, rows):
        own_copy(dr).wait_recv()
    sampled(me, True)

    bit = views // 4
    while bit:
        for step in steps:
            if lowest(step) == 2 * bit:
                point_copy(step).wait_recv()
        for step in steps:
            if lowest(step) == bit and step != bit:
                point_copy(step).start()
        bit //= 2

    def hand_on(step):
        feat_copy(step).wait_recv()
        for copy in pass_copies(step):
            copy.start()

    def ready(step):
        if lowest(step) == 1:
            point_copy(step).wait_recv()
        for copy in pass_copies(step):
            copy.wait_recv()

    def sample(step):
        ready(step)
        sampled(paired(step), False)

    if views <= UNROLL:
        for step in range(1, views):
            hand_on(step)
        for step in range(1, views):
            sample(step)
    else:
        for step in range(1, views):
            hand_on(step)
        for step in range(1, views):
            ready(step)
        pl.loop(1, views)(lambda step: sampled(paired(step), False))

    def backward(v):
        row, span, _, _, over = points(v)
        size = 2 * half
        crossing = [jnp.zeros((half, SPAN), F32)] * (spans - 1)
        for k in range(lines):
            grad = cotg[k] * (warp[v, k] - wsum[k] / views)
            spread = jnp.concatenate([grad * row_weight(row, k, h) for h in range(height)], axis=0)
            both = split(spread, 0)
            for t in range(spans):
                mask = jnp.where(span[k : k + 1] == float(t), 1.0, 0.0)
                moved[t * size : (t + 1) * size, k * width : (k + 1) * width] = both * mask.astype(BF16)
                if t < spans - 1:
                    beyond = spread * (mask * over[k : k + 1])
                    for n in range(0, width, SPAN):
                        crossing[t] = crossing[t] + beyond[:, n : n + SPAN]
        total = lax.dot_general(
            moved[...], mats[v], (((1,), (1,)), ((), ())), preferred_element_type=F32
        )
        starts = lax.broadcasted_iota(jnp.int32, (half, SPAN), 1) == 0
        for t in range(spans):
            part = total[t * size : t * size + half] + total[t * size + half : (t + 1) * size]
            if t:
                part = part + jnp.where(starts, jnp.sum(crossing[t - 1], axis=1, keepdims=True), 0.0)
            x, left = t * SPAN // wx, t * SPAN % wx
            for s in range(rows):
                for i in range(rl):
                    at = (s * rl + i) * cc
                    outbuf[v, s, x, :, i, left : left + SPAN] = part[at : at + cc]

    def core_copy(v, dr):
        r = row_at(dr)
        return pltpu.make_async_remote_copy(
            src_ref=outbuf.at[v, r], dst_ref=pbuf.at[v, dr],
            send_sem=d_send.at[v, dr], recv_sem=d_recv.at[v, dr],
            device_id={"row": r}, device_id_type=MESH,
        )

    def out_copy(v, step, dx):
        x = depth_at(dx)
        return pltpu.make_async_remote_copy(
            src_ref=red.at[v, x], dst_ref=inbuf.at[me, mx],
            send_sem=o_send.at[step, dx], recv_sem=o_recv.at[step, dx],
            device_id={"view": v, "depth": x}, device_id_type=MESH,
        )

    def add_cores(v):
        piece = outbuf[v, mr]
        for dr in range(1, rows):
            core_copy(v, dr).wait_recv()
            piece = piece + pbuf[v, dr]
        red[v] = piece

    def other_at(at):
        return at - 1 + (at - 1 + views - me) // views

    def pass_on(v):
        add_cores(v)
        for dx in range(depths):
            out_copy(v, paired(v), dx).start()

    @pl.loop(1, views)
    def _(at):
        v = other_at(at)
        backward(v)
        for dr in range(1, rows):
            core_copy(v, dr).start()

        @pl.when(at > 1)
        def _():
            pass_on(other_at(at - 1))

    backward(me)
    for dr in range(1, rows):
        core_copy(me, dr).start()
    if views > 1:
        pass_on(other_at(views - 1))
    add_cores(me)
    for dx in range(1, depths):
        out_copy(me, 0, dx).start()
    inbuf[me, mx] = red[me, mx]

    def arrived(step):
        for dx in range(depths):
            out_copy(paired(step), step, dx).wait_recv()

    for step in steps:
        arrived(step)
    for dx in range(1, depths):
        out_copy(me, 0, dx).wait_recv()
    for u in range(views):
        piece = inbuf[u, 0]
        for x in range(1, depths):
            piece = piece + inbuf[u, x]
        out[u * cc : (u + 1) * cc] = piece

    for dr in range(1, rows):
        own_copy(dr).wait_send()
        core_copy(me, dr).wait_send()
    for dx in range(1, depths):
        out_copy(me, 0, dx).wait_send()

    def finish(step):
        feat_copy(step).wait_send()
        point_copy(step).wait_send()
        for copy in pass_copies(step):
            copy.wait_send()
        for dr in range(1, rows):
            core_copy(paired(step), dr).wait_send()
        for dx in range(depths):
            out_copy(paired(step), step, dx).wait_send()

    for step in steps:
        finish(step)


def per_device(features, cotangent, src_row, src_col, fractions):
    views, depths, rows = (lax.axis_size(axis) for axis in ("view", "depth", "row"))
    channels, rl, width = features.shape[1:]
    planes, cc = cotangent.shape[:2]
    height, wx = rows * rl, width // depths
    lines = planes * rl
    spans = width // SPAN
    sizes = (views, depths, rows, cc, planes, rl, width)
    grad = pl.pallas_call(
        functools.partial(kernel, sizes),
        out_shape=pltpu.VMEM((channels, rl, wx), F32),
        in_specs=[pl.BlockSpec(memory_space=pl.ANY)] * 5,
        out_specs=pl.BlockSpec(memory_space=pltpu.VMEM),
        scratch_shapes=[
            pltpu.VMEM((views, rows, cc, rl, width), F32),
            pltpu.VMEM((planes, rl, width), jnp.int32),
            pltpu.VMEM((planes, rl, width), jnp.int32),
            pltpu.VMEM((2, planes, rl, width), jnp.int32),
            pltpu.VMEM((views, 2, lines, width), F32),
            pltpu.VMEM((planes, cc, rl, width), F32),
            pltpu.VMEM((lines, cc, width), F32),
            pltpu.VMEM((height * spans * cc, 2 * SPAN), BF16),
            pltpu.VMEM((height, max(spans - 1, 1), cc, COLS), F32),
            pltpu.VMEM((views, SPAN, lines * width), BF16),
            pltpu.VMEM((2 * height * spans * cc, lines * width), BF16),
            pltpu.VMEM((views, lines, cc, width), F32),
            pltpu.VMEM((lines, cc, width), F32),
            pltpu.VMEM((views, rows, depths, cc, rl, wx), F32),
            pltpu.VMEM((views, rows, depths, cc, rl, wx), F32),
            pltpu.VMEM((views, depths, cc, rl, wx), F32),
            pltpu.VMEM((views, depths, cc, rl, wx), F32),
            pltpu.SemaphoreType.DMA((5,)),
            pltpu.SemaphoreType.DMA((views,)),
            pltpu.SemaphoreType.DMA((views,)),
            pltpu.SemaphoreType.DMA((views, rows)),
            pltpu.SemaphoreType.DMA((views, rows)),
            pltpu.SemaphoreType.DMA((views,)),
            pltpu.SemaphoreType.DMA((views,)),
            pltpu.SemaphoreType.DMA((views, rows)),
            pltpu.SemaphoreType.DMA((views, rows)),
            pltpu.SemaphoreType.DMA((views, depths)),
            pltpu.SemaphoreType.DMA((views, depths)),
        ],
        compiler_params=pltpu.CompilerParams(
            collective_id=0, has_side_effects=True, vmem_limit_bytes=60 << 20
        ),
    )(features, cotangent, src_row, src_col, fractions)
    return grad[None]


def solution(mesh):
    in_specs = (
        P("view", None, ("group", "row"), None),
        P("depth", "view", ("group", "row"), None),
        P("view", "depth", ("group", "row"), None),
        P("view", "depth", ("group", "row"), None),
        P(None, "view", "depth", ("group", "row"), None),
    )
    out_specs = P("view", None, ("group", "row"), "depth")
    return jax.shard_map(
        per_device, mesh=mesh, in_specs=in_specs, out_specs=out_specs, check_vma=False
    )
```

```python
import functools

import jax
import jax.numpy as jnp
from jax import lax
from jax.experimental import pallas as pl
from jax.experimental.pallas import tpu as pltpu
from jax.sharding import PartitionSpec as P

MESH = pl.DeviceIdType.MESH
F32 = jnp.float32
BF16 = jnp.bfloat16
SPAN = 128
COLS = 256
UNROLL = 4


def split(value, axis):
    high = value.astype(BF16)
    low = (value - high.astype(F32)).astype(BF16)
    return jnp.concatenate([high, low], axis=axis)


def kernel(
    sizes, feat, cot, srow, scol, frac, out,
    fbuf, sbuf, qbuf, wbuf, cbuf, cotv, cotg, flat, edge, mats, moved, warp, wsum, outbuf, pbuf, red, inbuf,
    local_sem, f_send, f_recv, p_send, p_recv, i_send, i_recv, d_send, d_recv, o_send, o_recv,
):
    views, depths, rows, cc, planes, rl, width = sizes
    me = lax.axis_index("view")
    mx = lax.axis_index("depth")
    mr = lax.axis_index("row")
    height = rows * rl
    wx = width // depths
    lines = planes * rl
    spans = width // SPAN
    half = height * cc
    factor = 2.0 / views
    siblings = [(dx, dr) for dx in range(depths) for dr in range(rows) if dx or dr]

    def row_at(step):
        return lax.rem(mr + step, rows)

    def depth_at(step):
        return lax.rem(mx + step, depths)

    def step_of(at):
        return views - at

    steps = [step_of(at) for at in range(1, views)]

    def paired(step):
        other, bit = 0, 1
        while bit < views:
            other = other + bit * lax.rem(me // bit + step // bit, 2)
            bit *= 2
        return other

    def lowest(step):
        return step & -step

    barrier = pltpu.get_barrier_semaphore()

    def greet(v, x, r):
        pl.semaphore_signal(
            barrier, inc=1, device_id={"view": v, "depth": x, "row": r}, device_id_type=MESH
        )

    for step in steps:
        greet(paired(step), mx, mr)
    for dx in range(1, depths):
        for step in steps:
            greet(paired(step), depth_at(dx), mr)
        greet(me, depth_at(dx), mr)
    for dr in range(1, rows):
        greet(me, mx, row_at(dr))

    local = [
        pltpu.make_async_copy(srow.at[0], sbuf, local_sem.at[0]),
        pltpu.make_async_copy(scol.at[0], qbuf, local_sem.at[1]),
        pltpu.make_async_copy(frac.at[:, 0], wbuf, local_sem.at[2]),
        pltpu.make_async_copy(feat.at[0, pl.ds(me * cc, cc)], fbuf.at[me, mr], local_sem.at[3]),
        pltpu.make_async_copy(cot, cotv, local_sem.at[4]),
    ]
    for copy in local:
        copy.start()

    def feat_copy(step):
        to = paired(step)
        return pltpu.make_async_remote_copy(
            src_ref=feat.at[0, pl.ds(to * cc, cc)], dst_ref=fbuf.at[me, mr],
            send_sem=f_send.at[step], recv_sem=f_recv.at[step],
            device_id={"view": to}, device_id_type=MESH,
        )

    def own_copy(dr):
        return pltpu.make_async_remote_copy(
            src_ref=feat.at[0, pl.ds(me * cc, cc)], dst_ref=fbuf.at[me, mr],
            send_sem=p_send.at[0, dr], recv_sem=p_recv.at[0, dr],
            device_id={"row": row_at(dr)}, device_id_type=MESH,
        )

    def pass_copies(step):
        block = fbuf.at[paired(step), mr]
        return [
            pltpu.make_async_remote_copy(
                src_ref=block, dst_ref=block,
                send_sem=p_send.at[step, dr], recv_sem=p_recv.at[step, dr],
                device_id={"row": row_at(dr)}, device_id_type=MESH,
            )
            for dr in range(1, rows)
        ]

    def point_copy(step):
        block = cbuf.at[paired(step - lowest(step))]
        return pltpu.make_async_remote_copy(
            src_ref=block, dst_ref=block,
            send_sem=i_send.at[step], recv_sem=i_recv.at[step],
            device_id={"view": paired(lowest(step))}, device_id_type=MESH,
        )

    for copy in local[:3]:
        copy.wait()
    for d in range(planes):
        at = pl.ds(d * rl, rl)
        cbuf[me, 0, at, :] = sbuf[d].astype(F32) + wbuf[0, d].astype(F32) / 256.0
        cbuf[me, 1, at, :] = qbuf[d].astype(F32) + wbuf[1, d].astype(F32) / 256.0

    pl.semaphore_wait(barrier, views * depths + rows - 2)
    own_points = [step for step in steps if step == lowest(step)]
    for step in own_points:
        point_copy(step).start()
    for dr in range(1, rows):
        own_copy(dr).start()
    for step in range(1, views):
        feat_copy(step).start()

    lane = lax.broadcasted_iota(jnp.int32, (SPAN, COLS), 0).astype(F32).astype(BF16)

    def points(v):
        position = cbuf[v, 1]
        span = jnp.zeros_like(position)
        for t in range(1, spans):
            span = span + jnp.where(position >= float(t * SPAN), 1.0, 0.0)
        inside = position - span * float(SPAN)
        whole = jnp.floor(inside)
        rest = inside - whole
        return cbuf[v, 0], span, whole, rest, jnp.where(whole == float(SPAN - 1), rest, 0.0)

    def row_weight(row, k, h):
        return jnp.maximum(1.0 - jnp.abs(row[k : k + 1] - float(h)), 0.0)

    def flatten(v):
        parts = []
        for h in range(height):
            line = fbuf[v, h // rl, :, h % rl, :]
            for t in range(spans):
                parts.append(line[:, t * SPAN : (t + 1) * SPAN])
                if t:
                    first = line[:, t * SPAN : t * SPAN + 1]
                    edge[h, t - 1] = jnp.broadcast_to(first, (cc, COLS))
        flat[...] = split(jnp.concatenate(parts, axis=0), 1)

    def sampled(v, first):
        flatten(v)
        row, span, whole, rest, over = points(v)
        for k in range(lines):
            for n in range(0, width, COLS):
                cols = slice(n, n + COLS)
                at = jnp.broadcast_to(whole[k : k + 1, cols].astype(BF16), (SPAN, COLS))
                past = jnp.broadcast_to(rest[k : k + 1, cols].astype(BF16), (SPAN, COLS))
                mat = jnp.maximum(BF16(1.0) - jnp.abs((lane - at) - past), BF16(0.0))
                mats[v, :, k * width + n : k * width + n + COLS] = mat
                mixed = jnp.dot(
                    flat[...], jnp.concatenate([mat, mat], axis=0), preferred_element_type=F32
                )
                which = jnp.broadcast_to(span[k : k + 1, cols], (cc, COLS))
                beyond = jnp.broadcast_to(over[k : k + 1, cols], (cc, COLS))
                warped = None
                for h in range(height):
                    base = h * spans * cc
                    part, tail = mixed[base : base + cc], edge[h, 0] if spans > 1 else None
                    for t in range(1, spans):
                        here = base + t * cc
                        inside = which == float(t)
                        part = jnp.where(inside, mixed[here : here + cc], part)
                        if t < spans - 1:
                            tail = jnp.where(inside, edge[h, t], tail)
                    if tail is not None:
                        part = part + beyond * tail
                    part = part * row_weight(row, k, h)[:, cols]
                    warped = part if warped is None else warped + part
                warp[v, k, :, cols] = warped
                wsum[k, :, cols] = warped if first else wsum[k, :, cols] + warped

    local[4].wait()
    for k in range(lines):
        cotg[k] = factor * cotv[k // rl, :, k % rl, :]
    local[3].wait()
    for dr in range(1, rows):
        own_copy(dr).wait_recv()
    sampled(me, True)

    bit = views // 4
    while bit:
        for step in steps:
            if lowest(step) == 2 * bit:
                point_copy(step).wait_recv()
        for step in steps:
            if lowest(step) == bit and step != bit:
                point_copy(step).start()
        bit //= 2

    def hand_on(step):
        feat_copy(step).wait_recv()
        for copy in pass_copies(step):
            copy.start()

    def ready(step):
        if lowest(step) == 1:
            point_copy(step).wait_recv()
        for copy in pass_copies(step):
            copy.wait_recv()

    def sample(step):
        ready(step)
        sampled(paired(step), False)

    if views <= UNROLL:
        for step in range(1, views):
            hand_on(step)
        for step in range(1, views):
            sample(step)
    else:
        for step in range(1, views):
            hand_on(step)
        for step in range(1, views):
            ready(step)
        pl.loop(1, views)(lambda step: sampled(paired(step), False))

    def backward(v):
        row, span, _, _, over = points(v)
        size = 2 * half
        crossing = [jnp.zeros((half, SPAN), F32)] * (spans - 1)
        for k in range(lines):
            grad = cotg[k] * (warp[v, k] - wsum[k] / views)
            spread = jnp.concatenate([grad * row_weight(row, k, h) for h in range(height)], axis=0)
            both = split(spread, 0)
            for t in range(spans):
                mask = jnp.where(span[k : k + 1] == float(t), 1.0, 0.0)
                moved[t * size : (t + 1) * size, k * width : (k + 1) * width] = both * mask.astype(BF16)
                if t < spans - 1:
                    beyond = spread * (mask * over[k : k + 1])
                    for n in range(0, width, SPAN):
                        crossing[t] = crossing[t] + beyond[:, n : n + SPAN]
        total = lax.dot_general(
            moved[...], mats[v], (((1,), (1,)), ((), ())), preferred_element_type=F32
        )
        starts = lax.broadcasted_iota(jnp.int32, (half, SPAN), 1) == 0
        for t in range(spans):
            part = total[t * size : t * size + half] + total[t * size + half : (t + 1) * size]
            if t:
                part = part + jnp.where(starts, jnp.sum(crossing[t - 1], axis=1, keepdims=True), 0.0)
            x, left = t * SPAN // wx, t * SPAN % wx
            for s in range(rows):
                for i in range(rl):
                    at = (s * rl + i) * cc
                    outbuf[v, s, x, :, i, left : left + SPAN] = part[at : at + cc]

    def core_copy(v, dr):
        r = row_at(dr)
        return pltpu.make_async_remote_copy(
            src_ref=outbuf.at[v, r], dst_ref=pbuf.at[v, dr],
            send_sem=d_send.at[v, dr], recv_sem=d_recv.at[v, dr],
            device_id={"row": r}, device_id_type=MESH,
        )

    def out_copy(v, step, dx):
        x = depth_at(dx)
        return pltpu.make_async_remote_copy(
            src_ref=red.at[v, x], dst_ref=inbuf.at[me, mx],
            send_sem=o_send.at[step, dx], recv_sem=o_recv.at[step, dx],
            device_id={"view": v, "depth": x}, device_id_type=MESH,
        )

    def add_cores(v):
        piece = outbuf[v, mr]
        for dr in range(1, rows):
            core_copy(v, dr).wait_recv()
            piece = piece + pbuf[v, dr]
        red[v] = piece

    def pass_on(v):
        add_cores(v)
        for dx in range(1, depths):
            out_copy(v, paired(v), dx).start()

        @pl.when(v != me)
        def _():
            out_copy(v, paired(v), 0).start()

    def view_at(at):
        return lax.rem(at + (views - me) // views * (views - at - at), views)

    @pl.loop(0, views + 1)
    def _(at):
        @pl.when(at < views)
        def _():
            v = view_at(at)
            backward(v)
            for dr in range(1, rows):
                core_copy(v, dr).start()

        @pl.when(at > 0)
        def _():
            pass_on(view_at(at - 1))

    inbuf[me, mx] = red[me, mx]

    def arrived(step):
        for dx in range(depths):
            out_copy(paired(step), step, dx).wait_recv()

    for step in steps:
        arrived(step)
    for dx in range(1, depths):
        out_copy(me, 0, dx).wait_recv()
    for u in range(views):
        piece = inbuf[u, 0]
        for x in range(1, depths):
            piece = piece + inbuf[u, x]
        out[u * cc : (u + 1) * cc] = piece

    for dr in range(1, rows):
        own_copy(dr).wait_send()
        core_copy(me, dr).wait_send()
    for dx in range(1, depths):
        out_copy(me, 0, dx).wait_send()

    def finish(step):
        feat_copy(step).wait_send()
        point_copy(step).wait_send()
        for copy in pass_copies(step):
            copy.wait_send()
        for dr in range(1, rows):
            core_copy(paired(step), dr).wait_send()
        for dx in range(depths):
            out_copy(paired(step), step, dx).wait_send()

    for step in steps:
        finish(step)


def per_device(features, cotangent, src_row, src_col, fractions):
    views, depths, rows = (lax.axis_size(axis) for axis in ("view", "depth", "row"))
    channels, rl, width = features.shape[1:]
    planes, cc = cotangent.shape[:2]
    height, wx = rows * rl, width // depths
    lines = planes * rl
    spans = width // SPAN
    sizes = (views, depths, rows, cc, planes, rl, width)
    grad = pl.pallas_call(
        functools.partial(kernel, sizes),
        out_shape=pltpu.VMEM((channels, rl, wx), F32),
        in_specs=[pl.BlockSpec(memory_space=pl.ANY)] * 5,
        out_specs=pl.BlockSpec(memory_space=pltpu.VMEM),
        scratch_shapes=[
            pltpu.VMEM((views, rows, cc, rl, width), F32),
            pltpu.VMEM((planes, rl, width), jnp.int32),
            pltpu.VMEM((planes, rl, width), jnp.int32),
            pltpu.VMEM((2, planes, rl, width), jnp.int32),
            pltpu.VMEM((views, 2, lines, width), F32),
            pltpu.VMEM((planes, cc, rl, width), F32),
            pltpu.VMEM((lines, cc, width), F32),
            pltpu.VMEM((height * spans * cc, 2 * SPAN), BF16),
            pltpu.VMEM((height, max(spans - 1, 1), cc, COLS), F32),
            pltpu.VMEM((views, SPAN, lines * width), BF16),
            pltpu.VMEM((2 * height * spans * cc, lines * width), BF16),
            pltpu.VMEM((views, lines, cc, width), F32),
            pltpu.VMEM((lines, cc, width), F32),
            pltpu.VMEM((views, rows, depths, cc, rl, wx), F32),
            pltpu.VMEM((views, rows, depths, cc, rl, wx), F32),
            pltpu.VMEM((views, depths, cc, rl, wx), F32),
            pltpu.VMEM((views, depths, cc, rl, wx), F32),
            pltpu.SemaphoreType.DMA((5,)),
            pltpu.SemaphoreType.DMA((views,)),
            pltpu.SemaphoreType.DMA((views,)),
            pltpu.SemaphoreType.DMA((views, rows)),
            pltpu.SemaphoreType.DMA((views, rows)),
            pltpu.SemaphoreType.DMA((views,)),
            pltpu.SemaphoreType.DMA((views,)),
            pltpu.SemaphoreType.DMA((views, rows)),
            pltpu.SemaphoreType.DMA((views, rows)),
            pltpu.SemaphoreType.DMA((views, depths)),
            pltpu.SemaphoreType.DMA((views, depths)),
        ],
        compiler_params=pltpu.CompilerParams(
            collective_id=0, has_side_effects=True, vmem_limit_bytes=60 << 20
        ),
    )(features, cotangent, src_row, src_col, fractions)
    return grad[None]


def solution(mesh):
    in_specs = (
        P("view", None, ("group", "row"), None),
        P("depth", "view", ("group", "row"), None),
        P("view", "depth", ("group", "row"), None),
        P("view", "depth", ("group", "row"), None),
        P(None, "view", "depth", ("group", "row"), None),
    )
    out_specs = P("view", None, ("group", "row"), "depth")
    return jax.shard_map(
        per_device, mesh=mesh, in_specs=in_specs, out_specs=out_specs, check_vma=False
    )
```

```python
import functools

import jax
import jax.numpy as jnp
from jax import lax
from jax.experimental import pallas as pl
from jax.experimental.pallas import tpu as pltpu
from jax.sharding import PartitionSpec as P

MESH = pl.DeviceIdType.MESH
F32 = jnp.float32
BF16 = jnp.bfloat16
SPAN = 128
COLS = 256
UNROLL = 4


def split(value, axis):
    high = value.astype(BF16)
    low = (value - high.astype(F32)).astype(BF16)
    return jnp.concatenate([high, low], axis=axis)


def kernel(
    sizes, feat, cot, srow, scol, frac, out,
    fbuf, sbuf, qbuf, wbuf, cbuf, cotv, cotg, flat, edge, mats, moved, warp, wsum, outbuf, pbuf, red, inbuf,
    local_sem, f_send, f_recv, p_send, p_recv, i_send, i_recv, d_send, d_recv, o_send, o_recv,
):
    views, depths, rows, cc, planes, rl, width = sizes
    me = lax.axis_index("view")
    mx = lax.axis_index("depth")
    mr = lax.axis_index("row")
    height = rows * rl
    wx = width // depths
    lines = planes * rl
    spans = width // SPAN
    half = height * cc
    factor = 2.0 / views
    siblings = [(dx, dr) for dx in range(depths) for dr in range(rows) if dx or dr]

    def row_at(step):
        return lax.rem(mr + step, rows)

    def depth_at(step):
        return lax.rem(mx + step, depths)

    def step_of(at):
        return views - at

    steps = [step_of(at) for at in range(1, views)]

    def paired(step):
        other, bit = 0, 1
        while bit < views:
            other = other + bit * lax.rem(me // bit + step // bit, 2)
            bit *= 2
        return other

    def lowest(step):
        return step & -step

    barrier = pltpu.get_barrier_semaphore()

    def greet(v, x, r):
        pl.semaphore_signal(
            barrier, inc=1, device_id={"view": v, "depth": x, "row": r}, device_id_type=MESH
        )

    for step in steps:
        greet(paired(step), mx, mr)
    for dx in range(1, depths):
        for step in steps:
            greet(paired(step), depth_at(dx), mr)
        greet(me, depth_at(dx), mr)
    for dr in range(1, rows):
        greet(me, mx, row_at(dr))

    local = [
        pltpu.make_async_copy(srow.at[0], sbuf, local_sem.at[0]),
        pltpu.make_async_copy(scol.at[0], qbuf, local_sem.at[1]),
        pltpu.make_async_copy(frac.at[:, 0], wbuf, local_sem.at[2]),
        pltpu.make_async_copy(feat.at[0, pl.ds(me * cc, cc)], fbuf.at[me, mr], local_sem.at[3]),
        pltpu.make_async_copy(cot, cotv, local_sem.at[4]),
    ]
    for copy in local:
        copy.start()

    def feat_copy(step):
        to = paired(step)
        return pltpu.make_async_remote_copy(
            src_ref=feat.at[0, pl.ds(to * cc, cc)], dst_ref=fbuf.at[me, mr],
            send_sem=f_send.at[step], recv_sem=f_recv.at[step],
            device_id={"view": to}, device_id_type=MESH,
        )

    def own_copy(dr):
        return pltpu.make_async_remote_copy(
            src_ref=feat.at[0, pl.ds(me * cc, cc)], dst_ref=fbuf.at[me, mr],
            send_sem=p_send.at[0, dr], recv_sem=p_recv.at[0, dr],
            device_id={"row": row_at(dr)}, device_id_type=MESH,
        )

    def pass_copies(step):
        block = fbuf.at[paired(step), mr]
        return [
            pltpu.make_async_remote_copy(
                src_ref=block, dst_ref=block,
                send_sem=p_send.at[step, dr], recv_sem=p_recv.at[step, dr],
                device_id={"row": row_at(dr)}, device_id_type=MESH,
            )
            for dr in range(1, rows)
        ]

    def point_copy(step):
        block = cbuf.at[paired(step - lowest(step))]
        return pltpu.make_async_remote_copy(
            src_ref=block, dst_ref=block,
            send_sem=i_send.at[step], recv_sem=i_recv.at[step],
            device_id={"view": paired(lowest(step))}, device_id_type=MESH,
        )

    for copy in local[:3]:
        copy.wait()
    for d in range(planes):
        at = pl.ds(d * rl, rl)
        cbuf[me, 0, at, :] = sbuf[d].astype(F32) + wbuf[0, d].astype(F32) / 256.0
        cbuf[me, 1, at, :] = qbuf[d].astype(F32) + wbuf[1, d].astype(F32) / 256.0

    pl.semaphore_wait(barrier, views * depths + rows - 2)
    own_points = [step for step in steps if step == lowest(step)]
    for step in own_points:
        point_copy(step).start()
    for dr in range(1, rows):
        own_copy(dr).start()
    for step in range(1, views):
        feat_copy(step).start()

    lane = lax.broadcasted_iota(jnp.int32, (SPAN, COLS), 0).astype(F32).astype(BF16)

    def points(v):
        position = cbuf[v, 1]
        span = jnp.zeros_like(position)
        for t in range(1, spans):
            span = span + jnp.where(position >= float(t * SPAN), 1.0, 0.0)
        inside = position - span * float(SPAN)
        whole = jnp.floor(inside)
        rest = inside - whole
        return cbuf[v, 0], span, whole, rest, jnp.where(whole == float(SPAN - 1), rest, 0.0)

    def row_weight(row, k, h):
        return jnp.maximum(1.0 - jnp.abs(row[k : k + 1] - float(h)), 0.0)

    def flatten(v):
        parts = []
        for h in range(height):
            line = fbuf[v, h // rl, :, h % rl, :]
            for t in range(spans):
                parts.append(line[:, t * SPAN : (t + 1) * SPAN])
                if t:
                    first = line[:, t * SPAN : t * SPAN + 1]
                    edge[h, t - 1] = jnp.broadcast_to(first, (cc, COLS))
        flat[...] = split(jnp.concatenate(parts, axis=0), 1)

    def sampled(v, first):
        flatten(v)
        row, span, whole, rest, over = points(v)
        for k in range(lines):
            for n in range(0, width, COLS):
                cols = slice(n, n + COLS)
                at = jnp.broadcast_to(whole[k : k + 1, cols].astype(BF16), (SPAN, COLS))
                past = jnp.broadcast_to(rest[k : k + 1, cols].astype(BF16), (SPAN, COLS))
                mat = jnp.maximum(BF16(1.0) - jnp.abs((lane - at) - past), BF16(0.0))
                mats[v, :, k * width + n : k * width + n + COLS] = mat
                mixed = jnp.dot(
                    flat[...], jnp.concatenate([mat, mat], axis=0), preferred_element_type=F32
                )
                which = jnp.broadcast_to(span[k : k + 1, cols], (cc, COLS))
                beyond = jnp.broadcast_to(over[k : k + 1, cols], (cc, COLS))
                warped = None
                for h in range(height):
                    base = h * spans * cc
                    part, tail = mixed[base : base + cc], edge[h, 0] if spans > 1 else None
                    for t in range(1, spans):
                        here = base + t * cc
                        inside = which == float(t)
                        part = jnp.where(inside, mixed[here : here + cc], part)
                        if t < spans - 1:
                            tail = jnp.where(inside, edge[h, t], tail)
                    if tail is not None:
                        part = part + beyond * tail
                    part = part * row_weight(row, k, h)[:, cols]
                    warped = part if warped is None else warped + part
                warp[v, k, :, cols] = warped
                wsum[k, :, cols] = warped if first else wsum[k, :, cols] + warped

    local[3].wait()
    for dr in range(1, rows):
        own_copy(dr).wait_recv()
    sampled(me, True)

    bit = views // 4
    while bit:
        for step in steps:
            if lowest(step) == 2 * bit:
                point_copy(step).wait_recv()
        for step in steps:
            if lowest(step) == bit and step != bit:
                point_copy(step).start()
        bit //= 2

    def hand_on(step):
        feat_copy(step).wait_recv()
        for copy in pass_copies(step):
            copy.start()

    def ready(step):
        if lowest(step) == 1:
            point_copy(step).wait_recv()
        for copy in pass_copies(step):
            copy.wait_recv()

    def sample(step):
        ready(step)
        sampled(paired(step), False)

    local[4].wait()
    for k in range(lines):
        cotg[k] = factor * cotv[k // rl, :, k % rl, :]
    if views <= UNROLL:
        for step in range(1, views):
            hand_on(step)
        for step in range(1, views):
            sample(step)
    else:
        for step in range(1, views):
            hand_on(step)
        for step in range(1, views):
            ready(step)
        pl.loop(1, views)(lambda step: sampled(paired(step), False))

    def backward(v):
        row, span, _, _, over = points(v)
        size = 2 * half
        crossing = [jnp.zeros((half, SPAN), F32)] * (spans - 1)
        for k in range(lines):
            grad = cotg[k] * (warp[v, k] - wsum[k] / views)
            spread = jnp.concatenate([grad * row_weight(row, k, h) for h in range(height)], axis=0)
            both = split(spread, 0)
            for t in range(spans):
                mask = jnp.where(span[k : k + 1] == float(t), 1.0, 0.0)
                moved[t * size : (t + 1) * size, k * width : (k + 1) * width] = both * mask.astype(BF16)
                if t < spans - 1:
                    beyond = spread * (mask * over[k : k + 1])
                    for n in range(0, width, SPAN):
                        crossing[t] = crossing[t] + beyond[:, n : n + SPAN]
        total = lax.dot_general(
            moved[...], mats[v], (((1,), (1,)), ((), ())), preferred_element_type=F32
        )
        starts = lax.broadcasted_iota(jnp.int32, (half, SPAN), 1) == 0
        for t in range(spans):
            part = total[t * size : t * size + half] + total[t * size + half : (t + 1) * size]
            if t:
                part = part + jnp.where(starts, jnp.sum(crossing[t - 1], axis=1, keepdims=True), 0.0)
            x, left = t * SPAN // wx, t * SPAN % wx
            for s in range(rows):
                for i in range(rl):
                    at = (s * rl + i) * cc
                    outbuf[v, s, x, :, i, left : left + SPAN] = part[at : at + cc]

    def core_copy(v, dr):
        r = row_at(dr)
        return pltpu.make_async_remote_copy(
            src_ref=outbuf.at[v, r], dst_ref=pbuf.at[v, dr],
            send_sem=d_send.at[v, dr], recv_sem=d_recv.at[v, dr],
            device_id={"row": r}, device_id_type=MESH,
        )

    def out_copy(v, step, dx):
        x = depth_at(dx)
        return pltpu.make_async_remote_copy(
            src_ref=red.at[v, x], dst_ref=inbuf.at[me, mx],
            send_sem=o_send.at[step, dx], recv_sem=o_recv.at[step, dx],
            device_id={"view": v, "depth": x}, device_id_type=MESH,
        )

    def add_cores(v):
        piece = outbuf[v, mr]
        for dr in range(1, rows):
            core_copy(v, dr).wait_recv()
            piece = piece + pbuf[v, dr]
        red[v] = piece

    def pass_on(v):
        add_cores(v)
        for dx in range(1, depths):
            out_copy(v, paired(v), dx).start()

        @pl.when(v != me)
        def _():
            out_copy(v, paired(v), 0).start()

    def view_at(at):
        return lax.rem(at + (views - me) // views * (views - at - at), views)

    @pl.loop(0, views + 1)
    def _(at):
        @pl.when(at < views)
        def _():
            v = view_at(at)
            backward(v)
            for dr in range(1, rows):
                core_copy(v, dr).start()

        @pl.when(at > 0)
        def _():
            pass_on(view_at(at - 1))

    inbuf[me, mx] = red[me, mx]

    def arrived(step):
        for dx in range(depths):
            out_copy(paired(step), step, dx).wait_recv()

    for step in steps:
        arrived(step)
    for dx in range(1, depths):
        out_copy(me, 0, dx).wait_recv()
    for u in range(views):
        piece = inbuf[u, 0]
        for x in range(1, depths):
            piece = piece + inbuf[u, x]
        out[u * cc : (u + 1) * cc] = piece

    for dr in range(1, rows):
        own_copy(dr).wait_send()
        core_copy(me, dr).wait_send()
    for dx in range(1, depths):
        out_copy(me, 0, dx).wait_send()

    def finish(step):
        feat_copy(step).wait_send()
        point_copy(step).wait_send()
        for copy in pass_copies(step):
            copy.wait_send()
        for dr in range(1, rows):
            core_copy(paired(step), dr).wait_send()
        for dx in range(depths):
            out_copy(paired(step), step, dx).wait_send()

    for step in steps:
        finish(step)


def per_device(features, cotangent, src_row, src_col, fractions):
    views, depths, rows = (lax.axis_size(axis) for axis in ("view", "depth", "row"))
    channels, rl, width = features.shape[1:]
    planes, cc = cotangent.shape[:2]
    height, wx = rows * rl, width // depths
    lines = planes * rl
    spans = width // SPAN
    sizes = (views, depths, rows, cc, planes, rl, width)
    grad = pl.pallas_call(
        functools.partial(kernel, sizes),
        out_shape=pltpu.VMEM((channels, rl, wx), F32),
        in_specs=[pl.BlockSpec(memory_space=pl.ANY)] * 5,
        out_specs=pl.BlockSpec(memory_space=pltpu.VMEM),
        scratch_shapes=[
            pltpu.VMEM((views, rows, cc, rl, width), F32),
            pltpu.VMEM((planes, rl, width), jnp.int32),
            pltpu.VMEM((planes, rl, width), jnp.int32),
            pltpu.VMEM((2, planes, rl, width), jnp.int32),
            pltpu.VMEM((views, 2, lines, width), F32),
            pltpu.VMEM((planes, cc, rl, width), F32),
            pltpu.VMEM((lines, cc, width), F32),
            pltpu.VMEM((height * spans * cc, 2 * SPAN), BF16),
            pltpu.VMEM((height, max(spans - 1, 1), cc, COLS), F32),
            pltpu.VMEM((views, SPAN, lines * width), BF16),
            pltpu.VMEM((2 * height * spans * cc, lines * width), BF16),
            pltpu.VMEM((views, lines, cc, width), F32),
            pltpu.VMEM((lines, cc, width), F32),
            pltpu.VMEM((views, rows, depths, cc, rl, wx), F32),
            pltpu.VMEM((views, rows, depths, cc, rl, wx), F32),
            pltpu.VMEM((views, depths, cc, rl, wx), F32),
            pltpu.VMEM((views, depths, cc, rl, wx), F32),
            pltpu.SemaphoreType.DMA((5,)),
            pltpu.SemaphoreType.DMA((views,)),
            pltpu.SemaphoreType.DMA((views,)),
            pltpu.SemaphoreType.DMA((views, rows)),
            pltpu.SemaphoreType.DMA((views, rows)),
            pltpu.SemaphoreType.DMA((views,)),
            pltpu.SemaphoreType.DMA((views,)),
            pltpu.SemaphoreType.DMA((views, rows)),
            pltpu.SemaphoreType.DMA((views, rows)),
            pltpu.SemaphoreType.DMA((views, depths)),
            pltpu.SemaphoreType.DMA((views, depths)),
        ],
        compiler_params=pltpu.CompilerParams(
            collective_id=0, has_side_effects=True, vmem_limit_bytes=60 << 20
        ),
    )(features, cotangent, src_row, src_col, fractions)
    return grad[None]


def solution(mesh):
    in_specs = (
        P("view", None, ("group", "row"), None),
        P("depth", "view", ("group", "row"), None),
        P("view", "depth", ("group", "row"), None),
        P("view", "depth", ("group", "row"), None),
        P(None, "view", "depth", ("group", "row"), None),
    )
    out_specs = P("view", None, ("group", "row"), "depth")
    return jax.shard_map(
        per_device, mesh=mesh, in_specs=in_specs, out_specs=out_specs, check_vma=False
    )
```
